8 devices in a mesh: ep: 2 (over z, y), dp: 4 (over x, core).
Axes of the slice: x: 2, y: 2, z: 1, core: 2. Of those that a mesh axis runs over, the one named last changes fastest.
Arguments:
- act_in: bfloat16 [16384, 448], P(('ep', 'dp'))
- grad_out: bfloat16 [16384, 448], P(('ep', 'dp'))
- slot_ids: int32 [2, 16384, 8], P(None, ('ep', 'dp'))
- gate_vals: float32 [2, 16384, 8], P(None, ('ep', 'dp'))
- w_dense: bfloat16 [2, 448, 448], replicated
- w_gate: bfloat16 [2, 64, 448, 320], P(None, 'ep')
- w_up: bfloat16 [2, 64, 448, 320], P(None, 'ep')
- w_down: bfloat16 [2, 64, 320, 448], P(None, 'ep')
- ws_gate: bfloat16 [2, 448, 2560], replicated
- ws_up: bfloat16 [2, 448, 2560], replicated
- ws_down: bfloat16 [2, 2560, 448], replicated
Outputs:
- output 1: bfloat16 [16384, 448], P(('ep', 'dp'))
- output 2: bfloat16 [2, 448, 448], replicated
- output 3: bfloat16 [2, 64, 448, 320], P(None, 'ep')
- output 4: bfloat16 [2, 64, 448, 320], P(None, 'ep')
- output 5: bfloat16 [2, 64, 320, 448], P(None, 'ep')
- output 6: bfloat16 [2, 448, 2560], replicated
- output 7: bfloat16 [2, 448, 2560], replicated
- output 8: bfloat16 [2, 2560, 448], replicated
All inputs are finite; a program needn't handle non-finite values.
Results may differ from the reference program's by a relative error of at most 0.02.
Values are sent between devices in bfloat16 or wider.
A program may use at most 1 GiB of HBM per device.

```python
import functools
import jax
import jax.numpy as jnp
from jax import lax

D = 448
FF = 320
FS = 2560
EXPERTS = 64
TOP = 8
TOKENS = 2048
EP = 2
DP = 4
LAYERS = 2

NUM_DEV = EP * DP
CAP = 2 * TOKENS * TOP // EXPERTS
ROWS = NUM_DEV * TOKENS


def draw_slots(key):
    key_tok, key_exp = jax.random.split(key)
    mean_load = TOKENS * TOP // EXPERTS
    order = jax.random.permutation(key_tok, TOKENS)
    position = jnp.arange(TOP, dtype=jnp.int32)[None, :] * TOKENS + order[:, None]
    group = position // (4 * mean_load)
    rest = position % (4 * mean_load)
    first = 2 * mean_load
    second = first + mean_load // 2
    third = second + mean_load // 2
    within = (rest >= first).astype(jnp.int32) + (rest >= second).astype(jnp.int32) + (rest >= third).astype(jnp.int32)
    start = jnp.where(rest >= third, third, jnp.where(rest >= second, second, jnp.where(rest >= first, first, 0)))
    expert_perm = jax.random.permutation(key_exp, EXPERTS)
    expert = expert_perm[group * 4 + within]
    return (expert * CAP + rest - start).astype(jnp.int32)


def setup_inputs(seed: int = 0) -> dict:
    keys = jax.random.split(jax.random.key(seed), 12)
    slot_keys = jax.random.split(keys[0], LAYERS * NUM_DEV)
    slot_ids = jax.vmap(draw_slots)(slot_keys).reshape(LAYERS, ROWS, TOP)
    gate_vals = jax.random.uniform(keys[1], (LAYERS, ROWS, TOP), jnp.float32, 0.5, 1.5) / TOP
    act_in = jax.random.normal(keys[2], (ROWS, D), jnp.float32).astype(jnp.bfloat16)
    grad_out = jax.random.normal(keys[3], (ROWS, D), jnp.float32).astype(jnp.bfloat16)
    w_dense = (jax.random.normal(keys[4], (LAYERS, D, D), jnp.float32) * D ** -0.5).astype(jnp.bfloat16)
    w_gate = (jax.random.normal(keys[5], (LAYERS, EXPERTS, D, FF), jnp.float32) * D ** -0.5).astype(jnp.bfloat16)
    w_up = (jax.random.normal(keys[6], (LAYERS, EXPERTS, D, FF), jnp.float32) * D ** -0.5).astype(jnp.bfloat16)
    w_down = (jax.random.normal(keys[7], (LAYERS, EXPERTS, FF, D), jnp.float32) * FF ** -0.5).astype(jnp.bfloat16)
    ws_gate = (jax.random.normal(keys[8], (LAYERS, D, FS), jnp.float32) * D ** -0.5).astype(jnp.bfloat16)
    ws_up = (jax.random.normal(keys[9], (LAYERS, D, FS), jnp.float32) * D ** -0.5).astype(jnp.bfloat16)
    ws_down = (jax.random.normal(keys[10], (LAYERS, FS, D), jnp.float32) * FS ** -0.5).astype(jnp.bfloat16)
    return {"act_in": act_in, "grad_out": grad_out, "slot_ids": slot_ids, "gate_vals": gate_vals, "w_dense": w_dense, "w_gate": w_gate, "w_up": w_up, "w_down": w_down, "ws_gate": ws_gate, "ws_up": ws_up, "ws_down": ws_down}


def expert_block(args, w_gate32, w_up32, w_down32):
    mixed_loc, slot_loc, gate_loc = args
    slot_flat = slot_loc.reshape(TOKENS * TOP)
    copies = jnp.broadcast_to(mixed_loc[:, None, :], (TOKENS, TOP, D)).reshape(TOKENS * TOP, D)
    dispatched = jnp.zeros((EXPERTS * CAP, D), mixed_loc.dtype).at[slot_flat].set(copies)
    dispatched = dispatched.reshape(EXPERTS, CAP, D).astype(jnp.float32)
    a_one = jnp.einsum("ecd,edf->ecf", dispatched, w_gate32)
    a_three = jnp.einsum("ecd,edf->ecf", dispatched, w_up32)
    hidden = (jax.nn.silu(a_one) * a_three).astype(jnp.bfloat16)
    exp_out = jnp.einsum("ecf,efd->ecd", hidden.astype(jnp.float32), w_down32).astype(jnp.bfloat16)
    picked = exp_out.reshape(EXPERTS * CAP, D)[slot_flat].reshape(TOKENS, TOP, D)
    return jnp.sum(gate_loc[:, :, None] * picked.astype(jnp.float32), axis=1)


def moe_layer(act, layer_in):
    w_dense, w_gate, w_up, w_down, ws_gate, ws_up, ws_down, slot_ids, gate_vals = layer_in
    dense_pre = jnp.dot(act, w_dense, preferred_element_type=jnp.float32)
    mixed = (act.astype(jnp.float32) + dense_pre).astype(jnp.bfloat16)
    s_one = jnp.dot(mixed, ws_gate, preferred_element_type=jnp.float32)
    s_three = jnp.dot(mixed, ws_up, preferred_element_type=jnp.float32)
    shared_hidden = (jax.nn.silu(s_one) * s_three).astype(jnp.bfloat16)
    shared_out = jnp.dot(shared_hidden, ws_down, preferred_element_type=jnp.float32)
    block = jax.checkpoint(functools.partial(expert_block, w_gate32=w_gate.astype(jnp.float32), w_up32=w_up.astype(jnp.float32), w_down32=w_down.astype(jnp.float32)))
    routed = lax.map(block, (mixed.reshape(NUM_DEV, TOKENS, D), slot_ids.reshape(NUM_DEV, TOKENS, TOP), gate_vals.reshape(NUM_DEV, TOKENS, TOP)))
    routed = routed.reshape(ROWS, D)
    new_act = (mixed.astype(jnp.float32) + routed + shared_out).astype(jnp.bfloat16)
    return new_act, None


def reference(act_in, grad_out, slot_ids, gate_vals, w_dense, w_gate, w_up, w_down, ws_gate, ws_up, ws_down):
    def forward(act, dense_all, gate_all, up_all, down_all, sgate_all, sup_all, sdown_all):
        final, _ = lax.scan(moe_layer, act, (dense_all, gate_all, up_all, down_all, sgate_all, sup_all, sdown_all, slot_ids, gate_vals))
        return final
    _, pullback = jax.vjp(forward, act_in, w_dense, w_gate, w_up, w_down, ws_gate, ws_up, ws_down)
    grads = pullback(grad_out)
    return (grads[0], grads[1], grads[2], grads[3], grads[4], grads[5], grads[6], grads[7])
```

```python
import functools
import jax
import jax.numpy as jnp
from jax import lax
from jax.experimental import pallas as pl
from jax.experimental.pallas import tpu as pltpu
from jax.sharding import PartitionSpec as P

ALL_AXES = ("ep", "dp")
F32 = jnp.float32
BF16 = jnp.bfloat16
TILE = 256
VMEM_MAX = 60 * 1024 * 1024


def dot(left, right, dims=((1,), (0,))):
    return lax.dot_general(left, right, (dims, ((), ())), preferred_element_type=F32)


def silu_grad(pre_act):
    sigma = jax.nn.sigmoid(pre_act)
    return sigma * (1.0 + pre_act * (1.0 - sigma))


def contract_rows(left, right):
    return dot(left, right, ((0,), (0,)))


def contract_cols(left, right):
    return dot(left, right, ((1,), (1,)))


def route_kernel(exp_ref, gate_ref, pos_ref, gmat_ref, cnt_ref):
    sources, top, tokens = exp_ref.shape
    local_exp = pos_ref.shape[1]
    block = 256
    upper = (lax.broadcasted_iota(jnp.int32, (block, block), 0) < lax.broadcasted_iota(jnp.int32, (block, block), 1)).astype(BF16)
    exp_iota = lax.broadcasted_iota(jnp.int32, (local_exp, block), 0)
    for src in range(sources):
        carry = jnp.zeros((local_exp, 1), F32)
        for start in range(0, tokens, block):
            member = jnp.zeros((local_exp, block), F32)
            gates = jnp.zeros((local_exp, block), F32)
            for j in range(top):
                hit = exp_ref[src, j:j + 1, start:start + block] == exp_iota
                member = member + jnp.where(hit, 1.0, 0.0)
                gates = gates + jnp.where(hit, gate_ref[src, j:j + 1, start:start + block], 0.0)
            before = dot(member.astype(BF16), upper) + carry
            pos_ref[src, :, start:start + block] = jnp.where(member > 0.0, before, -1.0).astype(jnp.int32)
            gmat_ref[src, :, start:start + block] = gates
            carry = carry + jnp.sum(member, axis=1, keepdims=True)
        cnt_ref[src] = jnp.broadcast_to(carry, cnt_ref.shape[1:]).astype(jnp.int32)


def route(exp_ids, gates, local_exp):
    sources, top, tokens = exp_ids.shape
    pos, gmat, cnt = pl.pallas_call(
        route_kernel,
        out_shape=(
            jax.ShapeDtypeStruct((sources, local_exp, tokens), jnp.int32),
            jax.ShapeDtypeStruct((sources, local_exp, tokens), F32),
            jax.ShapeDtypeStruct((sources, local_exp, 128), jnp.int32),
        ),
        cost_estimate=pl.CostEstimate(flops=2 * sources * local_exp * tokens * 256, bytes_accessed=4 * sources * local_exp * tokens * 2, transcendentals=0),
        name="route",
    )(exp_ids, gates)
    return pos, gmat, cnt[:, :, 0]


def pick_rows(pos_ref, src, exp, row0):
    pos = pos_ref[src, pl.ds(exp, 1), :]
    hit = pos == row0 + lax.broadcasted_iota(jnp.int32, (TILE, pos.shape[1]), 0)
    return jnp.where(hit, 1.0, 0.0).astype(BF16)


def row_tiles(cnt_ref, exp):
    tiles0 = (cnt_ref[0, exp] + TILE - 1) // TILE
    return tiles0, tiles0 + (cnt_ref[1, exp] + TILE - 1) // TILE


def forward_kernel(cnt_ref, pos_ref, gmat_ref, tok_ref, wg_ref, wu_ref, wd_ref, out_ref):
    exp = pl.program_id(0)

    @pl.when(exp == 0)
    def _():
        out_ref[...] = jnp.zeros_like(out_ref)

    tiles0, tiles = row_tiles(cnt_ref, exp)

    def step(q, _):
        src = (q >= tiles0).astype(jnp.int32)
        pick = pick_rows(pos_ref, src, exp, (q - src * tiles0) * TILE)
        rows = contract_cols(tok_ref[src], pick).astype(BF16)
        a_one = dot(wg_ref[0, 0], rows)
        a_three = dot(wu_ref[0, 0], rows)
        hidden = (a_one * jax.nn.sigmoid(a_one) * a_three).astype(BF16)
        o_rows = contract_rows(wd_ref[0, 0], hidden).astype(BF16)
        out_ref[src] += gmat_ref[src, pl.ds(exp, 1), :] * dot(o_rows, pick)
        return 0

    lax.fori_loop(0, tiles, step, 0)


def whole_spec(*shape):
    return pl.BlockSpec(shape, lambda e, c: (0,) * len(shape), pipeline_mode=pl.Buffered(1))


def layer_spec(layer, inner, width):
    return pl.BlockSpec((1, 1, inner, width), lambda e, c: (layer, e, 0, 0))


def expert_forward(layer, cnt, pos, gmat, tok, w_gate, w_up, w_down):
    sources, width, tokens = tok.shape
    _, local_exp, inner, _ = w_gate.shape
    rows = sources * tokens * 4
    return pl.pallas_call(
        forward_kernel,
        out_shape=jax.ShapeDtypeStruct((sources, width, tokens), F32),
        grid_spec=pltpu.PrefetchScalarGridSpec(
            num_scalar_prefetch=1,
            grid=(local_exp,),
            in_specs=[whole_spec(*pos.shape), whole_spec(*gmat.shape), whole_spec(*tok.shape)] + [layer_spec(layer, inner, width)] * 3,
            out_specs=whole_spec(sources, width, tokens),
        ),
        compiler_params=pltpu.CompilerParams(dimension_semantics=("arbitrary",), vmem_limit_bytes=VMEM_MAX),
        cost_estimate=pl.CostEstimate(flops=rows * width * (4 * tokens + 6 * inner), bytes_accessed=6 * local_exp * width * inner, transcendentals=rows * inner),
        name="expert_forward",
    )(cnt, pos, gmat, tok, w_gate, w_up, w_down)


def pack_rows(inner, width):
    full = width // 128
    return 3 * inner * full + 3 * inner * (width - full * 128) // 128


def backward_kernel(cnt_ref, pos_ref, gmat_ref, tok_ref, gy_ref, wg_ref, wu_ref, wd_ref, own_ref, peer_ref, pack_ref, acc_ref, wacc_ref):
    exp = pl.program_id(0)
    _, width, tokens = tok_ref.shape
    inner = wg_ref.shape[2]

    @pl.when(exp == 0)
    def _():
        acc_ref[...] = jnp.zeros_like(acc_ref)

    wacc_ref[...] = jnp.zeros_like(wacc_ref)
    tiles0, tiles = row_tiles(cnt_ref, exp)

    def step(q, _):
        src = (q >= tiles0).astype(jnp.int32)
        pick = pick_rows(pos_ref, src, exp, (q - src * tiles0) * TILE)
        gate = gmat_ref[src, pl.ds(exp, 1), :]
        high = gate.astype(BF16).astype(F32)
        mid = (gate - high).astype(BF16).astype(F32)
        low = gate - high - mid
        part = lax.broadcasted_iota(jnp.int32, (16, tokens), 0)
        gate_parts = jnp.where(part == 0, high, jnp.where(part == 1, mid, jnp.where(part == 2, low, 0.0))).astype(BF16)
        table = jnp.concatenate([tok_ref[src], gy_ref[src], gate_parts], axis=0)
        got = contract_cols(table, pick)
        rows = got[:width].astype(BF16)
        row_gate = jnp.sum(got[2 * width:], axis=0, keepdims=True)
        g_rows = (row_gate * got[width:2 * width]).astype(BF16)
        a_one = dot(wg_ref[0, 0], rows)
        a_three = dot(wu_ref[0, 0], rows)
        g_hidden = dot(wd_ref[0, 0], g_rows)
        sigma = jax.nn.sigmoid(a_one)
        silu = a_one * sigma
        hidden = (silu * a_three).astype(BF16)
        g_one = (g_hidden * a_three * (sigma * (1.0 + a_one * (1.0 - sigma)))).astype(BF16)
        g_three = (g_hidden * silu).astype(BF16)
        wacc_ref[:inner] += contract_cols(g_one, rows)
        wacc_ref[inner:2 * inner] += contract_cols(g_three, rows)
        wacc_ref[2 * inner:] += contract_cols(hidden, g_rows)
        g_x = (contract_rows(wg_ref[0, 0], g_one) + contract_rows(wu_ref[0, 0], g_three)).astype(BF16)
        acc_ref[src] += dot(g_x, pick)
        return 0

    lax.fori_loop(0, tiles, step, 0)
    full = width // 128
    size = 3 * inner
    for lane in range(full):
        pack_ref[0, lane * size:(lane + 1) * size, :] = wacc_ref[:, lane * 128:(lane + 1) * 128].astype(BF16)
    rest = wacc_ref[:, full * 128:].astype(BF16)
    pack_ref[0, full * size:, :] = jnp.concatenate([rest[:size // 2], rest[size // 2:]], axis=1)

    @pl.when(exp == pl.num_programs(0) - 1)
    def _():
        own_ref[...] = acc_ref[0]
        peer_ref[...] = acc_ref[1].astype(BF16)


def expert_backward(layer, cnt, pos, gmat, tok, gy, w_gate, w_up, w_down):
    sources, width, tokens = tok.shape
    _, local_exp, inner, _ = w_gate.shape
    rows = sources * tokens * 4
    packed = pack_rows(inner, width)
    return pl.pallas_call(
        backward_kernel,
        out_shape=(
            jax.ShapeDtypeStruct((width, tokens), F32),
            jax.ShapeDtypeStruct((width, tokens), BF16),
            jax.ShapeDtypeStruct((local_exp, packed, 128), BF16),
        ),
        grid_spec=pltpu.PrefetchScalarGridSpec(
            num_scalar_prefetch=1,
            grid=(local_exp,),
            in_specs=[whole_spec(*pos.shape), whole_spec(*gmat.shape), whole_spec(*tok.shape), whole_spec(*gy.shape)] + [layer_spec(layer, inner, width)] * 3,
            out_specs=[whole_spec(width, tokens), whole_spec(width, tokens), pl.BlockSpec((1, packed, 128), lambda e, c: (e, 0, 0))],
            scratch_shapes=[pltpu.VMEM((sources, width, tokens), F32), pltpu.VMEM((3 * inner, width), F32)],
        ),
        compiler_params=pltpu.CompilerParams(dimension_semantics=("arbitrary",), vmem_limit_bytes=VMEM_MAX),
        cost_estimate=pl.CostEstimate(flops=rows * width * (6 * tokens + 18 * inner), bytes_accessed=12 * local_exp * width * inner, transcendentals=rows * inner),
        name="expert_backward",
    )(cnt, pos, gmat, tok, gy, w_gate, w_up, w_down)


def unpack_kernel(place_ref, pack_ref, *refs):
    outs = refs[len(refs) // 2:]
    inner, width = outs[0].shape[2:]
    full = width // 128
    size = 3 * inner
    half = size // 2
    for which, out in enumerate(outs):
        first = which * inner
        for lane in range(full):
            out[0, 0, :, lane * 128:(lane + 1) * 128] = pack_ref[0, lane * size + first:lane * size + first + inner, :]
        for start in range(first, first + inner, inner // 2):
            col = (start // half) * 64
            row = full * size + start % half
            out[0, 0, start - first:start - first + inner // 2, full * 128:] = pack_ref[0, row:row + inner // 2, col:col + 64]


def unpack_into(layer, place, piece, outs):
    count = piece.shape[0]
    inner, width = outs[0].shape[2:]
    out_spec = pl.BlockSpec((1, 1, inner, width), lambda e, p: (layer, p[0] * count + e, 0, 0))
    return pl.pallas_call(
        unpack_kernel,
        out_shape=tuple(jax.ShapeDtypeStruct(out.shape, out.dtype) for out in outs),
        grid_spec=pltpu.PrefetchScalarGridSpec(
            num_scalar_prefetch=1,
            grid=(count,),
            in_specs=[pl.BlockSpec((1,) + piece.shape[1:], lambda e, p: (e, 0, 0))] + [pl.BlockSpec(memory_space=pl.ANY)] * len(outs),
            out_specs=[out_spec] * len(outs),
        ),
        input_output_aliases={2 + i: i for i in range(len(outs))},
        compiler_params=pltpu.CompilerParams(dimension_semantics=("arbitrary",)),
        cost_estimate=pl.CostEstimate(flops=4 * piece.size, bytes_accessed=4 * piece.size, transcendentals=0),
        name="unpack",
    )(place.reshape(1), piece, *outs)


def swap(value, axis, size, bit):
    return lax.ppermute(value, axis, [(i, i ^ bit) for i in range(size)])


def reduce_over_dp(part, dp_size):
    index = lax.axis_index("dp")
    bits = [1 << b for b in range(dp_size.bit_length() - 1)]
    for bit in bits:
        half = part.shape[0] // 2
        mine = ((index // bit) % 2) * half
        got = swap(lax.dynamic_slice_in_dim(part, half - mine, half), "dp", dp_size, bit)
        part = (lax.dynamic_slice_in_dim(part, mine, half).astype(F32) + got.astype(F32)).astype(BF16)
    pieces = [(part, index)]
    for bit in reversed(bits):
        pieces = pieces + [(swap(piece, "dp", dp_size, bit), place ^ bit) for piece, place in pieces]
    return pieces, bits


def place_of(place, bits):
    return sum(((place // bit) % 2) << (len(bits) - 1 - order) for order, bit in enumerate(bits))


def solution(mesh):
    ep_size = mesh.shape["ep"]
    dp_size = mesh.shape["dp"]
    tok_spec = P(ALL_AXES, None)
    route_spec = P(None, ALL_AXES, None)
    exp_spec = P(None, "ep", None, None)
    repl_spec = P(None, None, None)

    def body(act_in, grad_out, slot_ids, gate_vals, w_dense, w_gate, w_up, w_down, ws_gate, ws_up, ws_down):
        layers, tokens, top = slot_ids.shape
        local_exp, width, inner = w_gate.shape[1:]
        capacity = 2 * tokens * top // (local_exp * ep_size)
        ep_index = lax.axis_index("ep")
        to_peer = lambda value: swap(value, "ep", ep_size, 1)
        pair = lambda value: jnp.stack([value, to_peer(value)])

        w_gate_t = w_gate.swapaxes(2, 3)
        w_up_t = w_up.swapaxes(2, 3)
        slots = pair(slot_ids.swapaxes(1, 2) // capacity) - ep_index * local_exp
        gates = pair(gate_vals.swapaxes(1, 2))
        routes = [route(slots[:, layer], gates[:, layer], local_exp) for layer in range(layers)]
        grad_y = grad_out.T
        grad2 = pair(grad_y)

        act = act_in.T
        saved = []
        for layer in range(layers):
            mixed = (act.astype(F32) + contract_rows(w_dense[layer], act)).astype(BF16)
            mixed2 = pair(mixed)
            s_one = contract_rows(ws_gate[layer], mixed)
            s_three = contract_rows(ws_up[layer], mixed)
            shared_hidden = (jax.nn.silu(s_one) * s_three).astype(BF16)
            saved.append((act, mixed, mixed2, s_one, s_three, shared_hidden))
            if layer + 1 < layers:
                pos, gmat, cnt = routes[layer]
                out = expert_forward(layer, cnt, pos, gmat, mixed2, w_gate_t, w_up_t, w_down)
                routed = out[0] + to_peer(out[1])
                act = (mixed.astype(F32) + routed + contract_rows(ws_down[layer], shared_hidden)).astype(BF16)

        dense_sums = [None] * layers
        expert_out = [jnp.zeros((layers, local_exp, inner, width), BF16) for _ in range(3)]
        for layer in reversed(range(layers)):
            act, mixed, mixed2, s_one, s_three, shared_hidden = saved[layer]
            pos, gmat, cnt = routes[layer]
            if layer + 1 < layers:
                grad2 = pair(grad_y)
            own, peer, packed = expert_backward(layer, cnt, pos, gmat, mixed2, grad2, w_gate_t, w_up_t, w_down)
            grad_routed = own + to_peer(peer).astype(F32)
            g_ws_down = contract_cols(shared_hidden, grad_y)
            grad_shared = dot(ws_down[layer], grad_y)
            grad_s_one = (grad_shared * s_three * silu_grad(s_one)).astype(BF16)
            grad_s_three = (grad_shared * jax.nn.silu(s_one)).astype(BF16)
            g_ws_gate = contract_cols(mixed, grad_s_one)
            g_ws_up = contract_cols(mixed, grad_s_three)
            grad_mixed = (grad_y.astype(F32) + grad_routed + dot(ws_gate[layer], grad_s_one) + dot(ws_up[layer], grad_s_three)).astype(BF16)
            g_w_dense = contract_cols(act, grad_mixed)
            grad_y = (grad_mixed.astype(F32) + dot(w_dense[layer], grad_mixed)).astype(BF16)
            dense_sums[layer] = [lax.psum(part.astype(BF16), ALL_AXES) for part in (g_w_dense, g_ws_gate, g_ws_up, g_ws_down)]
            pieces, bits = reduce_over_dp(packed, dp_size)
            for piece, place in pieces:
                expert_out = unpack_into(layer, place_of(place, bits), piece, expert_out)
        dense_out = [jnp.stack([dense_sums[layer][which] for layer in range(layers)]) for which in range(4)]
        return (grad_y.T, dense_out[0], expert_out[0].swapaxes(2, 3), expert_out[1].swapaxes(2, 3), expert_out[2], dense_out[1], dense_out[2], dense_out[3])

    return jax.shard_map(body, mesh=mesh, in_specs=(tok_spec, tok_spec, route_spec, route_spec, repl_spec, exp_spec, exp_spec, exp_spec, repl_spec, repl_spec, repl_spec), out_specs=(tok_spec, repl_spec, exp_spec, exp_spec, exp_spec, repl_spec, repl_spec, repl_spec), check_vma=False)
```
